32 devices in a mesh: seq: 8 (over y, x, core), head: 4 (over z).
Axes of the slice: x: 2, y: 2, z: 4, core: 2. Of those that a mesh axis runs over, the one named last changes fastest.
Arguments:
- queries: bfloat16 [4096, 4096], P('seq', 'head'), may hold values from -72 to 72
- key_heads: bfloat16 [4096, 4096], P('seq', 'head'), may hold values from -6 to 6
- value_heads: bfloat16 [4096, 4096], P('seq', 'head'), may hold values from -6 to 6
- dilation: int32 [4], replicated, may hold values from 1 to 8, as said below
- window: int32 [4], replicated, may hold values from 96 to 192, as said below
Outputs:
- attended: bfloat16 [4096, 4096], P('seq', 'head')
The draws below stay inside these ranges and needn't reach their ends.
Inputs may be any that keep to these rules, and one draw needn't show every extreme that they name: dilation holds the four numbers 1, 2, 4, 8, each once. Each window lies between 96 and 192; the group whose dilation is 8 has exactly 192.
All inputs are finite; a program needn't handle non-finite values.
Results may differ from the reference program's by a relative error of at most 0.0043.
Values may be sent and summed in bfloat16 or wider, within the bound.
A program may use at most 64 MiB of HBM per device.

```python
from functools import partial
import jax
import jax.numpy as jnp
from jax import lax

HEADS = 32
HS = 128
WIN = 192
GROUPS = 4
TOKENS = 4096


def group_draw(key):
    levels = jax.random.permutation(jax.random.fold_in(key, 11), GROUPS).astype(jnp.int32)
    dilation = jnp.left_shift(jnp.ones((GROUPS,), jnp.int32), levels)
    spans = jax.random.randint(jax.random.fold_in(key, 12), (GROUPS,), WIN // 2, WIN + 1, dtype=jnp.int32)
    spans = jnp.where(dilation == 8, WIN, spans).astype(jnp.int32)
    return (dilation, spans)


def draw_dilation(key, part):
    return group_draw(key)[0]


def draw_window(key, part):
    return group_draw(key)[1]


def key_draw(key):
    return jnp.clip(jax.random.normal(jax.random.fold_in(key, 21), (TOKENS, HEADS * HS), jnp.float32), -6.0, 6.0)


def draw_key_heads(key, part):
    return key_draw(key).astype(jnp.bfloat16)


def draw_queries(key, part):
    mixed = jnp.clip(jax.random.normal(jax.random.fold_in(key, 22), (TOKENS, HEADS * HS), jnp.float32), -6.0, 6.0)
    return mixed.astype(jnp.bfloat16)


def shard_levels(stream_key, dims, cuts, low, largest):
    factor_of, own = 1.0, jax.random.fold_in(stream_key, 6)
    for dim, shards_of in cuts:
        draws = jnp.exp(jax.random.uniform(jax.random.fold_in(own, dim), (shards_of,), jnp.float32, low / len(cuts), largest / len(cuts)))
        factor_of = factor_of * jnp.repeat(draws, dims[dim] // shards_of).reshape([-1 if axis == dim else 1 for axis in range(len(dims))])
    return factor_of


def noise(key, dims, scale, reach, cuts=(), kind=jnp.bfloat16):
    gain = shard_levels(key, dims, cuts, -0.22, 0.18) if cuts else 1.0
    result = jax.random.normal(key, dims, jnp.float32) * scale * gain
    return jnp.minimum(jnp.maximum(result, -reach), reach).astype(kind)


def setup_inputs(seed: int = 0) -> dict:
    keys = jax.random.split(jax.random.key(seed), 6)
    queries = draw_queries(jax.random.fold_in(keys[5], 71), 0)
    key_heads = draw_key_heads(jax.random.fold_in(keys[5], 71), 0)
    value_heads = noise(keys[2], (TOKENS, HEADS * HS), 1.0, 6.0, ((0, 8), (1, 4)))
    dilation = draw_dilation(jax.random.fold_in(keys[5], 71), 0)
    window = draw_window(jax.random.fold_in(keys[5], 71), 0)
    return dict(queries=queries, key_heads=key_heads, value_heads=value_heads, dilation=dilation, window=window)


masked_fill = -1.0e30


def group_attend(queries, key_heads, value_heads, reach_keys, degree):
    stride = 2 ** degree
    length, width = queries.shape
    heads_here = width // HS
    padding = jnp.zeros((stride * WIN, width), key_heads.dtype)
    keys_full = jnp.concatenate([padding, key_heads], axis=0)
    values_full = jnp.concatenate([padding, value_heads], axis=0)
    block_rows = min(512, length)
    per_class = block_rows // stride
    class_length = length // stride
    q_split = queries.reshape(class_length, stride, heads_here, HS)
    k_split = keys_full.reshape(class_length + WIN, stride, heads_here, HS)
    v_split = values_full.reshape(class_length + WIN, stride, heads_here, HS)
    scale = HS ** -0.5

    def one_block(number):
        opening = (number * per_class).astype(jnp.int32)
        q_block = lax.dynamic_slice_in_dim(q_split, opening, per_class, 0).astype(jnp.float32)
        k_block = lax.dynamic_slice_in_dim(k_split, opening, per_class + WIN, 0).astype(jnp.float32)
        v_block = lax.dynamic_slice_in_dim(v_split, opening, per_class + WIN, 0).astype(jnp.float32)
        scores = jnp.einsum("urhs,vrhs->rhuv", q_block, k_block) * scale
        query_index = jnp.arange(per_class, dtype=jnp.int32)[:, None]
        key_index = jnp.arange(per_class + WIN, dtype=jnp.int32)[None, :]
        distance = query_index - key_index + WIN
        inside = (distance >= 0) & (distance < reach_keys)
        position = -stride * WIN + (opening + key_index) * stride + jnp.arange(stride, dtype=jnp.int32)[:, None]
        valid = inside[None, None, :, :] & (position >= 0)[:, None, None, :]
        masked = jnp.where(valid, scores, masked_fill)
        peak = jnp.max(masked, axis=-1, keepdims=True)
        weights = jnp.where(valid, jnp.exp(masked - peak), 0.0)
        denominator = jnp.sum(weights, axis=-1)
        rounded = weights.astype(jnp.bfloat16)
        mixed = jnp.einsum("rhuv,vrhs->urhs", rounded.astype(jnp.float32), v_block)
        mixed = mixed / jnp.transpose(denominator, (2, 0, 1))[..., None]
        return mixed.astype(jnp.bfloat16).reshape(block_rows, width)

    blocks_out = lax.map(one_block, jnp.arange(length // block_rows, dtype=jnp.int32))
    return blocks_out.reshape(length, width)


def reference(queries, key_heads, value_heads, dilation, window):
    width = queries.shape[1]
    portion = width // GROUPS
    results = []
    for member in range(GROUPS):
        lower = member * portion
        upper = lower + portion
        level_index = ((dilation[member] > 1).astype(jnp.int32) + (dilation[member] > 2).astype(jnp.int32) + (dilation[member] > 4).astype(jnp.int32))
        branches = [partial(group_attend, degree=degree) for degree in range(4)]
        results.append(lax.switch(level_index, branches, queries[:, lower:upper], key_heads[:, lower:upper], value_heads[:, lower:upper], window[member]))
    return jnp.concatenate(results, axis=1)
```

```python
import functools
import math

import jax
import jax.numpy as jnp
from jax import lax
from jax.experimental import pallas as pl
from jax.experimental.pallas import tpu as pltpu
from jax.sharding import PartitionSpec as P

HS = 128
WIN = 192
MOST = 8
BACK = 3
masked_fill = -1e30
MESH = pl.DeviceIdType.MESH


def kernel(
    n,
    chunks,
    dil_ref,
    win_ref,
    q_ref,
    k_ref,
    v_ref,
    o_ref,
    slots,
    own,
    qv,
    ov,
    perm,
    perm_t,
    kvp,
    qp,
    op,
    send_sem,
    recv_sem,
    local_sem,
    out_sem,
):
    length, width = q_ref.shape
    cw = width // chunks
    tile = length // MOST
    behind = -(-WIN // tile)
    me = lax.axis_index("seq")
    core = me % 2
    chip = me // 2
    chips = n // 2
    partner = me + 1 - 2 * core
    wide = math.isqrt(chips)

    def wraps(c):
        return (c % wide == wide - 1) & (c + 2 < chips)

    detour_source = (core == 1) & wraps(chip)
    detour_via = (core == 0) & (chip >= 2) & ((chip - 2) % wide == wide - 1)

    barrier = pltpu.get_barrier_semaphore()
    near = [(step, (me + step >= 0) & (me + step < n)) for step in (-3, -2, -1, 1, 2, 3)]
    for step, there in near:

        @pl.when(there)
        def _():
            pl.semaphore_signal(barrier, inc=1, device_id={"seq": me + step}, device_id_type=MESH)

    pl.semaphore_wait(barrier, jnp.minimum(me, BACK) + jnp.minimum(n - 1 - me, BACK))

    def columns(j):
        return pl.ds(pl.multiple_of(j * cw, cw), cw)

    def place(slot, j, part):
        return slots.at[slot, j, :, pl.ds(part * cw, cw)]

    def remote(kind, src, slot, target, j, part):
        return pltpu.make_async_remote_copy(
            src_ref=src,
            dst_ref=place(slot, j, part),
            send_sem=send_sem.at[kind, j, part],
            recv_sem=recv_sem.at[slot, j, part],
            device_id={"seq": target},
            device_id_type=MESH,
        )

    def mine(kind, slot, step, j, part):
        src = (k_ref, v_ref)[part].at[:, columns(j)]
        return remote(kind, src, slot, me + step, j, part)

    def forward(j, part, which):
        slot = (2, 0)[which]
        return remote(3, place(1, j, part), slot, partner, j, part)

    def detour(j, part):
        return remote(4, place(2, j, part), 1, me - 1, j, part)

    def arrive(slot, j):
        for part in range(2):
            remote(0, place(slot, j, part), slot, partner, j, part).wait_recv()

    outgoing = [
        (1, 1, 2, (me + 2 < n) & jnp.logical_not(detour_source)),
        (2, 2, 3, (core == 1) & (me + 3 < n)),
        (0, 0, 1, core == 0),
    ]

    def local(j):
        return [
            pltpu.make_async_copy(q_ref.at[:, columns(j)], qv.at[j], local_sem.at[0, j]),
            pltpu.make_async_copy(
                k_ref.at[:, columns(j)], own.at[j, :, pl.ds(0, cw)], local_sem.at[1, j]
            ),
            pltpu.make_async_copy(
                v_ref.at[:, columns(j)], own.at[j, :, pl.ds(cw, cw)], local_sem.at[2, j]
            ),
        ]

    def result(j):
        return pltpu.make_async_copy(ov.at[j], o_ref.at[:, columns(j)], out_sem.at[j])

    def begin(j, carry):
        for kind, slot, step, there in outgoing:

            @pl.when(there)
            def _():
                for part in range(2):
                    mine(kind, slot, step, j, part).start()

        for copy in local(j):
            copy.start()
        return carry

    lax.fori_loop(0, chunks, begin, 0)

    for slot in range(BACK):

        @pl.when(me < slot + 1)
        def _():
            slots[slot] = jnp.zeros(slots.shape[1:], slots.dtype)

    group = lax.axis_index("head")
    dilation = dil_ref[group]
    reach = win_ref[group]
    level = (
        (dilation > 1).astype(jnp.int32)
        + (dilation > 2).astype(jnp.int32)
        + (dilation > 4).astype(jnp.int32)
    )
    per_class = length >> level
    row = lax.broadcasted_iota(jnp.int32, (length, length), 0)
    col = lax.broadcasted_iota(jnp.int32, (length, length), 1)

    def target_of(token):
        return (token & (dilation - 1)) * per_class + (token >> level)

    perm[...] = jnp.where(row == target_of(col), 1.0, 0.0).astype(jnp.bfloat16)
    perm_t[...] = jnp.where(col == target_of(row), 1.0, 0.0).astype(jnp.bfloat16)

    span = (behind + 1) * tile
    apart = (
        lax.broadcasted_iota(jnp.int32, (tile, span), 0)
        - lax.broadcasted_iota(jnp.int32, (tile, span), 1)
        + behind * tile
    )
    key_at = lax.broadcasted_iota(jnp.int32, (tile, span), 1)
    inside = (apart >= 0) & (apart < reach)
    scale = HS ** (-0.5)

    def by_level(four):
        pick = jnp.where(dilation > 1, four[1], four[0])
        pick = jnp.where(dilation > 2, four[2], pick)
        return jnp.where(dilation > 4, four[3], pick)

    tiles_here = by_level([MOST, MOST // 2, MOST // 4, MOST // 8])

    def sort_rows(x):
        return jnp.dot(perm[...], x, preferred_element_type=jnp.float32).astype(jnp.bfloat16)

    def fetch(j):
        @pl.when((core == 0) & (chip >= 2))
        def _():
            arrive(2, j)

        @pl.when(detour_via)
        def _():
            for part in range(2):
                detour(j, part).start()

        @pl.when(chip >= 1)
        def _():
            arrive(1, j)

        for which in range(2):

            @pl.when((chip >= 1) & (core == which))
            def _():
                for part in range(2):
                    forward(j, part, which).start()

    def compute(j):
        @pl.when((core == 1) | (chip >= 1))
        def _():
            arrive(0, j)

        @pl.when((core == 1) & (chip >= 1))
        def _():
            arrive(2, j)

        for copy in local(j):
            copy.wait()
        qp[...] = sort_rows(qv[j]).reshape(qp.shape)
        kvp[pl.ds(0, MOST)] = sort_rows(own[j]).reshape(MOST, tile, 2 * cw)
        for slot in range(BACK):
            kvp[pl.ds((slot + 1) * MOST, MOST)] = sort_rows(slots[slot, j]).reshape(
                MOST, tile, 2 * cw
            )
        for t in range(MOST):
            spots = []
            for offset in range(behind + 1):
                found = []
                for held in (MOST, MOST // 2, MOST // 4, MOST // 8):
                    back, at = divmod(t % held - behind + offset, held)
                    found.append(-back * MOST + t // held * held + at)
                spots.append(by_level(found))
            first = by_level([t % held for held in (MOST, MOST // 2, MOST // 4, MOST // 8)])
            valid = inside & (key_at >= tile * (behind - me * tiles_here - first))
            keys_values = jnp.concatenate([kvp[spot] for spot in spots], axis=0)
            for h in range(cw // HS):
                lanes = slice(h * HS, (h + 1) * HS)
                keys = keys_values[:, lanes]
                values = keys_values[:, cw + h * HS : cw + (h + 1) * HS]
                scores = (
                    lax.dot_general(
                        qp[t, :, lanes],
                        keys,
                        (((1,), (1,)), ((), ())),
                        preferred_element_type=jnp.float32,
                    )
                    * scale
                )
                masked = jnp.where(valid, scores, masked_fill)
                peak = jnp.max(masked, axis=-1, keepdims=True)
                weights = jnp.where(valid, jnp.exp(masked - peak), 0.0)
                total = jnp.sum(weights, axis=-1, keepdims=True)
                mixed = jnp.dot(
                    weights.astype(jnp.bfloat16), values, preferred_element_type=jnp.float32
                )
                op[pl.ds(t * tile, tile), lanes] = (mixed / total).astype(jnp.bfloat16)
        ov[j] = jnp.dot(perm_t[...], op[...], preferred_element_type=jnp.float32).astype(
            jnp.bfloat16
        )
        result(j).start()

    def turn(j, carry):
        @pl.when(j < chunks)
        def _():
            fetch(j)

        @pl.when(j >= 1)
        def _():
            compute(j - 1)

        return carry

    lax.fori_loop(0, chunks + 1, turn, 0)

    def finish(j, carry):
        for part in range(2):
            for kind, slot, step, there in outgoing:

                @pl.when(there)
                def _():
                    mine(kind, slot, step, j, part).wait_send()

            @pl.when(chip >= 1)
            def _():
                forward(j, part, 0).wait_send()

            @pl.when(detour_via)
            def _():
                detour(j, part).wait_send()

        result(j).wait()
        return carry

    lax.fori_loop(0, chunks, finish, 0)


def solution(mesh):
    n = mesh.shape["seq"]

    def body(queries, key_heads, value_heads, dilation, window):
        length, width = queries.shape
        chunks = width // HS
        cw = width // chunks
        tile = length // MOST
        half = jnp.bfloat16
        anywhere = pl.BlockSpec(memory_space=pl.ANY)
        scalars = pl.BlockSpec(memory_space=pltpu.SMEM)
        return pl.pallas_call(
            functools.partial(kernel, n, chunks),
            out_shape=jax.ShapeDtypeStruct((length, width), half),
            in_specs=[scalars, scalars, anywhere, anywhere, anywhere],
            out_specs=anywhere,
            scratch_shapes=[
                pltpu.VMEM((BACK, chunks, length, 2 * cw), half),
                pltpu.VMEM((chunks, length, 2 * cw), half),
                pltpu.VMEM((chunks, length, cw), half),
                pltpu.VMEM((chunks, length, cw), half),
                pltpu.VMEM((length, length), half),
                pltpu.VMEM((length, length), half),
                pltpu.VMEM(((BACK + 1) * MOST, tile, 2 * cw), half),
                pltpu.VMEM((MOST, tile, cw), half),
                pltpu.VMEM((length, cw), half),
                pltpu.SemaphoreType.DMA((5, chunks, 2)),
                pltpu.SemaphoreType.DMA((BACK, chunks, 2)),
                pltpu.SemaphoreType.DMA((3, chunks)),
                pltpu.SemaphoreType.DMA((chunks,)),
            ],
            compiler_params=pltpu.CompilerParams(collective_id=0, has_side_effects=True),
        )(dilation, window, queries, key_heads, value_heads)

    return jax.shard_map(
        body,
        mesh=mesh,
        in_specs=(P("seq", "head"), P("seq", "head"), P("seq", "head"), P(), P()),
        out_specs=P("seq", "head"),
        check_vma=False,
    )
```

```python
import functools
import math

import jax
import jax.numpy as jnp
from jax import lax
from jax.experimental import pallas as pl
from jax.experimental.pallas import tpu as pltpu
from jax.sharding import PartitionSpec as P

HS = 128
WIN = 192
MOST = 8
BACK = 3
masked_fill = -1e30
MESH = pl.DeviceIdType.MESH


def kernel(
    n,
    chunks,
    dil_ref,
    win_ref,
    q_ref,
    k_ref,
    v_ref,
    o_ref,
    slots,
    own,
    ov,
    perm,
    perm_t,
    sorted_rows,
    raw,
    rounded,
    totals,
    op,
    send_sem,
    recv_sem,
    local_sem,
    out_sem,
):
    length, width = q_ref.shape
    cw = width // chunks
    tile = length // MOST
    behind = -(-WIN // tile)
    me = lax.axis_index("seq")
    core = me % 2
    chip = me // 2
    chips = n // 2
    partner = me + 1 - 2 * core
    wide = math.isqrt(chips)

    def wraps(c):
        return (c % wide == wide - 1) & (c + 2 < chips)

    detour_source = (core == 1) & wraps(chip)
    detour_via = (core == 0) & (chip >= 2) & ((chip - 2) % wide == wide - 1)

    barrier = pltpu.get_barrier_semaphore()
    near = [(step, (me + step >= 0) & (me + step < n)) for step in (-3, -2, -1, 1, 2, 3)]
    for step, there in near:

        @pl.when(there)
        def _():
            pl.semaphore_signal(barrier, inc=1, device_id={"seq": me + step}, device_id_type=MESH)

    pl.semaphore_wait(barrier, jnp.minimum(me, BACK) + jnp.minimum(n - 1 - me, BACK))

    def columns(j):
        return pl.ds(pl.multiple_of(j * cw, cw), cw)

    def place(slot, j, part):
        return slots.at[slot, part, j]

    def remote(kind, src, slot, target, j, part):
        return pltpu.make_async_remote_copy(
            src_ref=src,
            dst_ref=place(slot, j, part),
            send_sem=send_sem.at[kind, j, part],
            recv_sem=recv_sem.at[slot, j, part],
            device_id={"seq": target},
            device_id_type=MESH,
        )

    def mine(kind, slot, step, j, part):
        src = (k_ref, v_ref)[part].at[:, columns(j)]
        return remote(kind, src, slot, me + step, j, part)

    def forward(j, part, which):
        slot = (2, 0)[which]
        return remote(3, place(1, j, part), slot, partner, j, part)

    def detour(j, part):
        return remote(4, place(2, j, part), 1, me - 1, j, part)

    def arrive(slot, j, part):
        remote(0, place(slot, j, part), slot, partner, j, part).wait_recv()

    outgoing = [
        (1, 1, 2, (me + 2 < n) & jnp.logical_not(detour_source)),
        (2, 2, 3, (core == 1) & (me + 3 < n)),
        (0, 0, 1, core == 0),
    ]

    def local(part, j):
        src = (k_ref, v_ref, q_ref)[part].at[:, columns(j)]
        return pltpu.make_async_copy(src, own.at[part, j], local_sem.at[part, j])

    def result(j):
        return pltpu.make_async_copy(ov.at[j], o_ref.at[:, columns(j)], out_sem.at[j])

    def begin(j, carry):
        for kind, slot, step, there in outgoing:

            @pl.when(there)
            def _():
                for part in range(2):
                    mine(kind, slot, step, j, part).start()

        for part in range(3):
            local(part, j).start()
        return carry

    lax.fori_loop(0, chunks, begin, 0)

    for slot in range(BACK):

        @pl.when(me < slot + 1)
        def _():
            slots[slot] = jnp.zeros(slots.shape[1:], slots.dtype)

    group = lax.axis_index("head")
    dilation = dil_ref[group]
    reach = win_ref[group]
    level = (
        (dilation > 1).astype(jnp.int32)
        + (dilation > 2).astype(jnp.int32)
        + (dilation > 4).astype(jnp.int32)
    )
    per_class = length >> level
    row = lax.broadcasted_iota(jnp.int32, (length, length), 0)
    col = lax.broadcasted_iota(jnp.int32, (length, length), 1)

    def target_of(token):
        return (token & (dilation - 1)) * per_class + (token >> level)

    perm[...] = jnp.where(row == target_of(col), 1.0, 0.0).astype(jnp.bfloat16)
    perm_t[...] = jnp.where(col == target_of(row), 1.0, 0.0).astype(jnp.bfloat16)

    span = (behind + 1) * tile
    apart = (
        lax.broadcasted_iota(jnp.int32, (tile, span), 0)
        - lax.broadcasted_iota(jnp.int32, (tile, span), 1)
        + behind * tile
    )
    key_at = lax.broadcasted_iota(jnp.int32, (tile, span), 1)
    inside = (apart >= 0) & (apart < reach)
    scale = HS ** (-0.5)

    def by_level(four):
        pick = jnp.where(dilation > 1, four[1], four[0])
        pick = jnp.where(dilation > 2, four[2], pick)
        return jnp.where(dilation > 4, four[3], pick)

    tiles_here = by_level([MOST, MOST // 2, MOST // 4, MOST // 8])

    def sort_rows(parts):
        joined = jnp.concatenate(parts, axis=1)
        moved = jnp.dot(perm[...], joined, preferred_element_type=jnp.float32)
        moved = moved.astype(jnp.bfloat16).reshape(MOST, tile, joined.shape[1])
        width_of = parts[0].shape[1]
        return [moved[:, :, i * width_of : (i + 1) * width_of] for i in range(len(parts))]

    def relay(j):
        @pl.when(detour_via)
        def _():
            for part in range(2):
                arrive(2, j, part)
                detour(j, part).start()

    def fetch(j, part):
        @pl.when(chip >= 1)
        def _():
            arrive(1, j, part)

        for which in range(2):

            @pl.when((chip >= 1) & (core == which))
            def _():
                forward(j, part, which).start()

        local(part, j).wait()
        near_rows, far_rows = sort_rows([own[part, j], slots[1, part, j]])
        sorted_rows[part, pl.ds(0, MOST)] = near_rows
        sorted_rows[part, pl.ds(2 * MOST, MOST)] = far_rows

    def complete(j, part):
        @pl.when((core == 1) | (chip >= 1))
        def _():
            arrive(0, j, part)

        @pl.when(((core == 0) & (chip >= 2) & jnp.logical_not(detour_via)) | ((core == 1) & (chip >= 1)))
        def _():
            arrive(2, j, part)

        near_rows, far_rows = sort_rows([slots[0, part, j], slots[2, part, j]])
        sorted_rows[part, pl.ds(MOST, MOST)] = near_rows
        sorted_rows[part, pl.ds(3 * MOST, MOST)] = far_rows

    levels_of = (MOST, MOST // 2, MOST // 4, MOST // 8)
    spots = []
    firsts = []
    for t in range(MOST):
        row_of = []
        for offset in range(behind + 1):
            found = []
            for held in levels_of:
                back, at = divmod(t % held - behind + offset, held)
                found.append(-back * MOST + t // held * held + at)
            row_of.append(by_level(found))
        spots.append(row_of)
        firsts.append(by_level([t % held for held in levels_of]))

    def rows_for(part, t):
        return jnp.concatenate([sorted_rows[part, spot] for spot in spots[t]], axis=0)

    heads = cw // HS

    def score(j):
        local(2, j).wait()
        (asked,) = sort_rows([own[2, j]])
        complete(j, 0)
        for t in range(MOST):
            keys = rows_for(0, t)
            for h in range(heads):
                lanes = slice(h * HS, (h + 1) * HS)
                raw[h, t] = lax.dot_general(
                    asked[t, :, lanes],
                    keys[:, lanes],
                    (((1,), (1,)), ((), ())),
                    preferred_element_type=jnp.float32,
                )
        for t in range(MOST):
            valid = inside & (key_at >= tile * (behind - me * tiles_here - firsts[t]))
            for h in range(heads):
                masked = jnp.where(valid, raw[h, t] * scale, masked_fill)
                weights = jnp.exp(masked - jnp.max(masked, axis=-1, keepdims=True))
                totals[h, t] = jnp.sum(weights, axis=-1, keepdims=True)
                rounded[h, t] = weights.astype(jnp.bfloat16)

    def mix(j):
        complete(j, 1)
        for t in range(MOST):
            values = rows_for(1, t)
            for h in range(heads):
                lanes = slice(h * HS, (h + 1) * HS)
                mixed = jnp.dot(
                    rounded[h, t], values[:, lanes], preferred_element_type=jnp.float32
                )
                op[pl.ds(t * tile, tile), lanes] = (mixed / totals[h, t]).astype(jnp.bfloat16)
        ov[j] = jnp.dot(perm_t[...], op[...], preferred_element_type=jnp.float32).astype(
            jnp.bfloat16
        )
        result(j).start()

    relay(0)

    def turn(j, carry):
        @pl.when(j < chunks - 1)
        def _():
            relay(j + 1)

        fetch(j, 0)

        @pl.when(j >= 1)
        def _():
            mix(j - 1)

        score(j)
        fetch(j, 1)
        return carry

    lax.fori_loop(0, chunks, turn, 0)
    mix(chunks - 1)

    def finish(j, carry):
        for part in range(2):
            for kind, slot, step, there in outgoing:

                @pl.when(there)
                def _():
                    mine(kind, slot, step, j, part).wait_send()

            @pl.when(chip >= 1)
            def _():
                forward(j, part, 0).wait_send()

            @pl.when(detour_via)
            def _():
                detour(j, part).wait_send()

        result(j).wait()
        return carry

    lax.fori_loop(0, chunks, finish, 0)


def solution(mesh):
    n = mesh.shape["seq"]

    def body(queries, key_heads, value_heads, dilation, window):
        length, width = queries.shape
        chunks = width // HS
        cw = width // chunks
        tile = length // MOST
        span = (-(-WIN // tile) + 1) * tile
        half = jnp.bfloat16
        anywhere = pl.BlockSpec(memory_space=pl.ANY)
        scalars = pl.BlockSpec(memory_space=pltpu.SMEM)
        return pl.pallas_call(
            functools.partial(kernel, n, chunks),
            out_shape=jax.ShapeDtypeStruct((length, width), half),
            in_specs=[scalars, scalars, anywhere, anywhere, anywhere],
            out_specs=anywhere,
            scratch_shapes=[
                pltpu.VMEM((BACK, 2, chunks, length, cw), half),
                pltpu.VMEM((3, chunks, length, cw), half),
                pltpu.VMEM((chunks, length, cw), half),
                pltpu.VMEM((length, length), half),
                pltpu.VMEM((length, length), half),
                pltpu.VMEM((2, (BACK + 1) * MOST, tile, cw), half),
                pltpu.VMEM((cw // HS, MOST, tile, span), jnp.float32),
                pltpu.VMEM((cw // HS, MOST, tile, span), half),
                pltpu.VMEM((cw // HS, MOST, tile, 1), jnp.float32),
                pltpu.VMEM((length, cw), half),
                pltpu.SemaphoreType.DMA((5, chunks, 2)),
                pltpu.SemaphoreType.DMA((BACK, chunks, 2)),
                pltpu.SemaphoreType.DMA((3, chunks)),
                pltpu.SemaphoreType.DMA((chunks,)),
            ],
            compiler_params=pltpu.CompilerParams(collective_id=0, has_side_effects=True),
        )(dilation, window, queries, key_heads, value_heads)

    return jax.shard_map(
        body,
        mesh=mesh,
        in_specs=(P("seq", "head"), P("seq", "head"), P("seq", "head"), P(), P()),
        out_specs=P("seq", "head"),
        check_vma=False,
    )
```

```python
import functools
import math

import jax
import jax.numpy as jnp
from jax import lax
from jax.experimental import pallas as pl
from jax.experimental.pallas import tpu as pltpu
from jax.sharding import PartitionSpec as P

HS = 128
WIN = 192
MOST = 8
BACK = 3
masked_fill = -1e30
MESH = pl.DeviceIdType.MESH


def kernel(
    n,
    chunks,
    dil_ref,
    win_ref,
    q_ref,
    k_ref,
    v_ref,
    o_ref,
    slots,
    own,
    perm,
    perm_t,
    sorted_rows,
    raw,
    rounded,
    totals,
    op,
    send_sem,
    recv_sem,
    local_sem,
):
    length, width = q_ref.shape
    cw = width // chunks
    tile = length // MOST
    behind = -(-WIN // tile)
    me = lax.axis_index("seq")
    core = me % 2
    chip = me // 2
    chips = n // 2
    partner = me + 1 - 2 * core
    wide = math.isqrt(chips)

    def wraps(c):
        return (c % wide == wide - 1) & (c + 2 < chips)

    detour_source = (core == 1) & wraps(chip)
    detour_via = (core == 0) & (chip >= 2) & ((chip - 2) % wide == wide - 1)

    barrier = pltpu.get_barrier_semaphore()
    near = [(step, (me + step >= 0) & (me + step < n)) for step in (-3, -2, -1, 1, 2, 3)]
    for step, there in near:

        @pl.when(there)
        def _():
            pl.semaphore_signal(barrier, inc=1, device_id={"seq": me + step}, device_id_type=MESH)

    pl.semaphore_wait(barrier, jnp.minimum(me, BACK) + jnp.minimum(n - 1 - me, BACK))

    def columns(j):
        return pl.ds(pl.multiple_of(j * cw, cw), cw)

    def place(slot, j, part):
        return slots.at[slot, part, j]

    def remote(kind, src, slot, target, j, part):
        return pltpu.make_async_remote_copy(
            src_ref=src,
            dst_ref=place(slot, j, part),
            send_sem=send_sem.at[kind, j, part],
            recv_sem=recv_sem.at[slot, j, part],
            device_id={"seq": target},
            device_id_type=MESH,
        )

    def mine(kind, slot, step, j, part):
        src = (k_ref, v_ref)[part].at[:, columns(j)]
        return remote(kind, src, slot, me + step, j, part)

    def forward(j, part, which):
        slot = (2, 0)[which]
        return remote(3, place(1, j, part), slot, partner, j, part)

    def detour(j, part):
        return remote(4, place(2, j, part), 1, me - 1, j, part)

    def arrive(slot, j, part):
        remote(0, place(slot, j, part), slot, partner, j, part).wait_recv()

    outgoing = [
        (1, 1, 2, (me + 2 < n) & jnp.logical_not(detour_source)),
        (2, 2, 3, (core == 1) & (me + 3 < n)),
        (0, 0, 1, core == 0),
    ]

    def local(part, j):
        src = (k_ref, v_ref, q_ref)[part].at[:, columns(j)]
        return pltpu.make_async_copy(src, own.at[part, j], local_sem.at[part, j])

    def begin(j, carry):
        for kind, slot, step, there in outgoing:

            @pl.when(there)
            def _():
                for part in range(2):
                    mine(kind, slot, step, j, part).start()

        for part in range(3):
            local(part, j).start()
        return carry

    lax.fori_loop(0, chunks, begin, 0)

    for slot in range(BACK):

        @pl.when(me < slot + 1)
        def _():
            slots[slot] = jnp.zeros(slots.shape[1:], slots.dtype)

    group = lax.axis_index("head")
    dilation = dil_ref[group]
    reach = win_ref[group]
    level = (
        (dilation > 1).astype(jnp.int32)
        + (dilation > 2).astype(jnp.int32)
        + (dilation > 4).astype(jnp.int32)
    )
    per_class = length >> level
    row = lax.broadcasted_iota(jnp.int32, (length, length), 0)
    col = lax.broadcasted_iota(jnp.int32, (length, length), 1)

    def target_of(token):
        return (token & (dilation - 1)) * per_class + (token >> level)

    perm[...] = jnp.where(row == target_of(col), 1.0, 0.0).astype(jnp.bfloat16)
    perm_t[...] = jnp.where(col == target_of(row), 1.0, 0.0).astype(jnp.bfloat16)

    span = (behind + 1) * tile
    apart = (
        lax.broadcasted_iota(jnp.int32, (tile, span), 0)
        - lax.broadcasted_iota(jnp.int32, (tile, span), 1)
        + behind * tile
    )
    key_at = lax.broadcasted_iota(jnp.int32, (tile, span), 1)
    inside = (apart >= 0) & (apart < reach)
    scale = HS ** (-0.5)

    def by_level(four):
        pick = jnp.where(dilation > 1, four[1], four[0])
        pick = jnp.where(dilation > 2, four[2], pick)
        return jnp.where(dilation > 4, four[3], pick)

    tiles_here = by_level([MOST, MOST // 2, MOST // 4, MOST // 8])

    def sort_rows(parts):
        joined = jnp.concatenate(parts, axis=1)
        moved = jnp.dot(perm[...], joined, preferred_element_type=jnp.float32)
        moved = moved.astype(jnp.bfloat16).reshape(MOST, tile, joined.shape[1])
        width_of = parts[0].shape[1]
        return [moved[:, :, i * width_of : (i + 1) * width_of] for i in range(len(parts))]

    def relay(j):
        @pl.when(detour_via)
        def _():
            for part in range(2):
                arrive(2, j, part)
                detour(j, part).start()

    def fetch(j, part):
        @pl.when(chip >= 1)
        def _():
            arrive(1, j, part)

        for which in range(2):

            @pl.when((chip >= 1) & (core == which))
            def _():
                forward(j, part, which).start()

        local(part, j).wait()
        near_rows, far_rows = sort_rows([own[part, j], slots[1, part, j]])
        sorted_rows[part, pl.ds(0, MOST)] = near_rows
        sorted_rows[part, pl.ds(2 * MOST, MOST)] = far_rows

    def complete(j, part):
        @pl.when((core == 1) | (chip >= 1))
        def _():
            arrive(0, j, part)

        @pl.when(((core == 0) & (chip >= 2) & jnp.logical_not(detour_via)) | ((core == 1) & (chip >= 1)))
        def _():
            arrive(2, j, part)

        near_rows, far_rows = sort_rows([slots[0, part, j], slots[2, part, j]])
        sorted_rows[part, pl.ds(MOST, MOST)] = near_rows
        sorted_rows[part, pl.ds(3 * MOST, MOST)] = far_rows

    levels_of = (MOST, MOST // 2, MOST // 4, MOST // 8)
    spots = []
    firsts = []
    for t in range(MOST):
        row_of = []
        for offset in range(behind + 1):
            found = []
            for held in levels_of:
                back, at = divmod(t % held - behind + offset, held)
                found.append(-back * MOST + t // held * held + at)
            row_of.append(by_level(found))
        spots.append(row_of)
        firsts.append(by_level([t % held for held in levels_of]))

    def rows_for(part, t):
        return jnp.concatenate([sorted_rows[part, spot] for spot in spots[t]], axis=0)

    heads = cw // HS

    def score(j):
        local(2, j).wait()
        (asked,) = sort_rows([own[2, j]])
        complete(j, 0)
        for t in range(MOST):
            keys = rows_for(0, t)
            for h in range(heads):
                lanes = slice(h * HS, (h + 1) * HS)
                raw[h, t] = lax.dot_general(
                    asked[t, :, lanes],
                    keys[:, lanes],
                    (((1,), (1,)), ((), ())),
                    preferred_element_type=jnp.float32,
                )
        for t in range(MOST):
            valid = inside & (key_at >= tile * (behind - me * tiles_here - firsts[t]))
            for h in range(heads):
                masked = jnp.where(valid, raw[h, t] * scale, masked_fill)
                weights = jnp.exp(masked - jnp.max(masked, axis=-1, keepdims=True))
                totals[h, t] = jnp.sum(weights, axis=-1, keepdims=True)
                rounded[h, t] = weights.astype(jnp.bfloat16)

    def mix(j):
        complete(j, 1)
        for t in range(MOST):
            values = rows_for(1, t)
            for h in range(heads):
                lanes = slice(h * HS, (h + 1) * HS)
                mixed = jnp.dot(
                    rounded[h, t], values[:, lanes], preferred_element_type=jnp.float32
                )
                op[pl.ds(t * tile, tile), lanes] = (mixed / totals[h, t]).astype(jnp.bfloat16)
        o_ref[:, columns(j)] = jnp.dot(
            perm_t[...], op[...], preferred_element_type=jnp.float32
        ).astype(jnp.bfloat16)

    relay(0)

    def turn(j, carry):
        @pl.when(j < chunks - 1)
        def _():
            relay(j + 1)

        fetch(j, 0)

        @pl.when(j >= 1)
        def _():
            mix(j - 1)

        score(j)
        fetch(j, 1)
        return carry

    lax.fori_loop(0, chunks, turn, 0)
    mix(chunks - 1)

    def finish(j, carry):
        for part in range(2):
            for kind, slot, step, there in outgoing:

                @pl.when(there)
                def _():
                    mine(kind, slot, step, j, part).wait_send()

            @pl.when(chip >= 1)
            def _():
                forward(j, part, 0).wait_send()

            @pl.when(detour_via)
            def _():
                detour(j, part).wait_send()

        return carry

    lax.fori_loop(0, chunks, finish, 0)


def solution(mesh):
    n = mesh.shape["seq"]

    def body(queries, key_heads, value_heads, dilation, window):
        length, width = queries.shape
        chunks = width // HS
        cw = width // chunks
        tile = length // MOST
        span = (-(-WIN // tile) + 1) * tile
        half = jnp.bfloat16
        hbm = pl.BlockSpec(memory_space=pltpu.HBM)
        scalars = pl.BlockSpec(memory_space=pltpu.SMEM)
        return pl.pallas_call(
            functools.partial(kernel, n, chunks),
            out_shape=pltpu.VMEM((length, width), half),
            in_specs=[scalars, scalars, hbm, hbm, hbm],
            out_specs=pl.BlockSpec(memory_space=pltpu.VMEM),
            scratch_shapes=[
                pltpu.VMEM((BACK, 2, chunks, length, cw), half),
                pltpu.VMEM((3, chunks, length, cw), half),
                pltpu.VMEM((length, length), half),
                pltpu.VMEM((length, length), half),
                pltpu.VMEM((2, (BACK + 1) * MOST, tile, cw), half),
                pltpu.VMEM((cw // HS, MOST, tile, span), jnp.float32),
                pltpu.VMEM((cw // HS, MOST, tile, span), half),
                pltpu.VMEM((cw // HS, MOST, tile, 1), jnp.float32),
                pltpu.VMEM((length, cw), half),
                pltpu.SemaphoreType.DMA((5, chunks, 2)),
                pltpu.SemaphoreType.DMA((BACK, chunks, 2)),
                pltpu.SemaphoreType.DMA((3, chunks)),
            ],
            compiler_params=pltpu.CompilerParams(
                collective_id=0, has_side_effects=True, vmem_limit_bytes=60 * 2**20
            ),
        )(dilation, window, queries, key_heads, value_heads)

    return jax.shard_map(
        body,
        mesh=mesh,
        in_specs=(P("seq", "head"), P("seq", "head"), P("seq", "head"), P(), P()),
        out_specs=P("seq", "head"),
        check_vma=False,
    )
```

```python
import functools
import math

import jax
import jax.numpy as jnp
from jax import lax
from jax.experimental import pallas as pl
from jax.experimental.pallas import tpu as pltpu
from jax.sharding import PartitionSpec as P

HS = 128
WIN = 192
MOST = 8
BACK = 3
masked_fill = -1e30
MESH = pl.DeviceIdType.MESH


def kernel(
    n,
    chunks,
    dil_ref,
    win_ref,
    q_ref,
    k_ref,
    v_ref,
    o_ref,
    slots,
    own,
    perm,
    perm_t,
    sorted_rows,
    raw,
    rounded,
    totals,
    op,
    send_sem,
    recv_sem,
    local_sem,
):
    length, width = q_ref.shape
    cw = width // chunks
    tile = length // MOST
    behind = -(-WIN // tile)
    me = lax.axis_index("seq")
    core = me % 2
    chip = me // 2
    chips = n // 2
    partner = me + 1 - 2 * core
    wide = math.isqrt(chips)

    def wraps(c):
        return (c % wide == wide - 1) & (c + 2 < chips)

    detour_source = (core == 1) & wraps(chip)
    detour_via = (core == 0) & (chip >= 2) & ((chip - 2) % wide == wide - 1)

    barrier = pltpu.get_barrier_semaphore()
    near = [(step, (me + step >= 0) & (me + step < n)) for step in (-3, -2, -1, 1, 2, 3)]
    for step, there in near:

        @pl.when(there)
        def _():
            pl.semaphore_signal(barrier, inc=1, device_id={"seq": me + step}, device_id_type=MESH)

    pl.semaphore_wait(barrier, jnp.minimum(me, BACK) + jnp.minimum(n - 1 - me, BACK))

    def columns(j):
        return pl.ds(pl.multiple_of(j * cw, cw), cw)

    def place(slot, j, part):
        return slots.at[slot, part, j]

    def remote(kind, src, slot, target, j, part):
        return pltpu.make_async_remote_copy(
            src_ref=src,
            dst_ref=place(slot, j, part),
            send_sem=send_sem.at[kind, j, part],
            recv_sem=recv_sem.at[slot, j, part],
            device_id={"seq": target},
            device_id_type=MESH,
        )

    def mine(kind, slot, step, j, part):
        src = (k_ref, v_ref)[part].at[:, columns(j)]
        return remote(kind, src, slot, me + step, j, part)

    def forward(j, part, which):
        slot = (2, 0)[which]
        return remote(3, place(1, j, part), slot, partner, j, part)

    def detour(j, part):
        return remote(4, place(2, j, part), 1, me - 1, j, part)

    def arrive(slot, j, part):
        remote(0, place(slot, j, part), slot, partner, j, part).wait_recv()

    outgoing = [
        (1, 1, 2, (me + 2 < n) & jnp.logical_not(detour_source)),
        (2, 2, 3, (core == 1) & (me + 3 < n)),
        (0, 0, 1, core == 0),
    ]

    def local(part, j):
        src = (k_ref, v_ref, q_ref)[part].at[:, columns(j)]
        return pltpu.make_async_copy(src, own.at[part, j], local_sem.at[part, j])

    def begin(j, carry):
        for kind, slot, step, there in outgoing:

            @pl.when(there)
            def _():
                for part in range(2):
                    mine(kind, slot, step, j, part).start()

        for part in range(3):
            local(part, j).start()
        return carry

    lax.fori_loop(0, chunks, begin, 0)

    for slot in range(BACK):

        @pl.when(me < slot + 1)
        def _():
            slots[slot] = jnp.zeros(slots.shape[1:], slots.dtype)

    group = lax.axis_index("head")
    dilation = dil_ref[group]
    reach = win_ref[group]
    level = (
        (dilation > 1).astype(jnp.int32)
        + (dilation > 2).astype(jnp.int32)
        + (dilation > 4).astype(jnp.int32)
    )
    per_class = length >> level
    row = lax.broadcasted_iota(jnp.int32, (length, length), 0)
    col = lax.broadcasted_iota(jnp.int32, (length, length), 1)

    def target_of(token):
        return (token & (dilation - 1)) * per_class + (token >> level)

    perm[...] = jnp.where(row == target_of(col), 1.0, 0.0).astype(jnp.bfloat16)
    perm_t[...] = jnp.where(col == target_of(row), 1.0, 0.0).astype(jnp.bfloat16)

    span = (behind + 1) * tile
    apart = (
        lax.broadcasted_iota(jnp.int32, (tile, span), 0)
        - lax.broadcasted_iota(jnp.int32, (tile, span), 1)
        + behind * tile
    )
    key_at = lax.broadcasted_iota(jnp.int32, (tile, span), 1)
    inside = (apart >= 0) & (apart < reach)
    scale = HS ** (-0.5)

    def by_level(four):
        pick = jnp.where(dilation > 1, four[1], four[0])
        pick = jnp.where(dilation > 2, four[2], pick)
        return jnp.where(dilation > 4, four[3], pick)

    tiles_here = by_level([MOST, MOST // 2, MOST // 4, MOST // 8])

    def sort_rows(parts):
        joined = jnp.concatenate(parts, axis=1)
        moved = jnp.dot(perm[...], joined, preferred_element_type=jnp.float32)
        moved = moved.astype(jnp.bfloat16).reshape(MOST, tile, joined.shape[1])
        width_of = parts[0].shape[1]
        return [moved[:, :, i * width_of : (i + 1) * width_of] for i in range(len(parts))]

    def relay(j):
        @pl.when(detour_via)
        def _():
            for part in range(2):
                arrive(2, j, part)
                detour(j, part).start()

    def fetch(j, part):
        @pl.when(chip >= 1)
        def _():
            arrive(1, j, part)

        for which in range(2):

            @pl.when((chip >= 1) & (core == which))
            def _():
                forward(j, part, which).start()

        local(part, j).wait()
        near_rows, far_rows = sort_rows([own[part, j], slots[1, part, j]])
        sorted_rows[part, pl.ds(0, MOST)] = near_rows
        sorted_rows[part, pl.ds(2 * MOST, MOST)] = far_rows

    def complete(j, part):
        @pl.when((core == 1) | (chip >= 1))
        def _():
            arrive(0, j, part)

        @pl.when(((core == 0) & (chip >= 2) & jnp.logical_not(detour_via)) | ((core == 1) & (chip >= 1)))
        def _():
            arrive(2, j, part)

        near_rows, far_rows = sort_rows([slots[0, part, j], slots[2, part, j]])
        sorted_rows[part, pl.ds(MOST, MOST)] = near_rows
        sorted_rows[part, pl.ds(3 * MOST, MOST)] = far_rows

    levels_of = (MOST, MOST // 2, MOST // 4, MOST // 8)
    spots = []
    firsts = []
    for t in range(MOST):
        row_of = []
        for offset in range(behind + 1):
            found = []
            for held in levels_of:
                back, at = divmod(t % held - behind + offset, held)
                found.append(-back * MOST + t // held * held + at)
            row_of.append(by_level(found))
        spots.append(row_of)
        firsts.append(by_level([t % held for held in levels_of]))

    def rows_for(part, t):
        return jnp.concatenate([sorted_rows[part, spot] for spot in spots[t]], axis=0)

    heads = cw // HS

    def score(j):
        local(2, j).wait()
        (asked,) = sort_rows([own[2, j]])
        complete(j, 0)
        for t in range(MOST):
            keys = rows_for(0, t)
            for h in range(heads):
                lanes = slice(h * HS, (h + 1) * HS)
                raw[h, t] = lax.dot_general(
                    asked[t, :, lanes],
                    keys[:, lanes],
                    (((1,), (1,)), ((), ())),
                    preferred_element_type=jnp.float32,
                )
        for t in range(MOST):
            valid = inside & (key_at >= tile * (behind - me * tiles_here - firsts[t]))
            for h in range(heads):
                masked = jnp.where(valid, raw[h, t] * scale, masked_fill)
                weights = jnp.exp(masked - jnp.max(masked, axis=-1, keepdims=True))
                totals[h, t] = jnp.sum(weights, axis=-1, keepdims=True)
                rounded[h, t] = weights.astype(jnp.bfloat16)

    def mix(j):
        complete(j, 1)
        for t in range(MOST):
            values = rows_for(1, t)
            for h in range(heads):
                lanes = slice(h * HS, (h + 1) * HS)
                mixed = jnp.dot(
                    rounded[h, t], values[:, lanes], preferred_element_type=jnp.float32
                )
                op[pl.ds(t * tile, tile), lanes] = (mixed / totals[h, t]).astype(jnp.bfloat16)
        o_ref[:, columns(j)] = jnp.dot(
            perm_t[...], op[...], preferred_element_type=jnp.float32
        ).astype(jnp.bfloat16)

    relay(0)

    def turn(j, carry):
        @pl.when(j < chunks - 1)
        def _():
            relay(j + 1)

        fetch(j, 0)

        @pl.when(j >= 1)
        def _():
            mix(j - 1)

        fetch(j, 1)
        score(j)
        return carry

    lax.fori_loop(0, chunks, turn, 0)
    mix(chunks - 1)

    def finish(j, carry):
        for part in range(2):
            for kind, slot, step, there in outgoing:

                @pl.when(there)
                def _():
                    mine(kind, slot, step, j, part).wait_send()

            @pl.when(chip >= 1)
            def _():
                forward(j, part, 0).wait_send()

            @pl.when(detour_via)
            def _():
                detour(j, part).wait_send()

        return carry

    lax.fori_loop(0, chunks, finish, 0)


def solution(mesh):
    n = mesh.shape["seq"]

    def body(queries, key_heads, value_heads, dilation, window):
        length, width = queries.shape
        chunks = width // HS
        cw = width // chunks
        tile = length // MOST
        span = (-(-WIN // tile) + 1) * tile
        half = jnp.bfloat16
        hbm = pl.BlockSpec(memory_space=pltpu.HBM)
        scalars = pl.BlockSpec(memory_space=pltpu.SMEM)
        return pl.pallas_call(
            functools.partial(kernel, n, chunks),
            out_shape=pltpu.VMEM((length, width), half),
            in_specs=[scalars, scalars, hbm, hbm, hbm],
            out_specs=pl.BlockSpec(memory_space=pltpu.VMEM),
            scratch_shapes=[
                pltpu.VMEM((BACK, 2, chunks, length, cw), half),
                pltpu.VMEM((3, chunks, length, cw), half),
                pltpu.VMEM((length, length), half),
                pltpu.VMEM((length, length), half),
                pltpu.VMEM((2, (BACK + 1) * MOST, tile, cw), half),
                pltpu.VMEM((cw // HS, MOST, tile, span), jnp.float32),
                pltpu.VMEM((cw // HS, MOST, tile, span), half),
                pltpu.VMEM((cw // HS, MOST, tile, 1), jnp.float32),
                pltpu.VMEM((length, cw), half),
                pltpu.SemaphoreType.DMA((5, chunks, 2)),
                pltpu.SemaphoreType.DMA((BACK, chunks, 2)),
                pltpu.SemaphoreType.DMA((3, chunks)),
            ],
            compiler_params=pltpu.CompilerParams(
                collective_id=0, has_side_effects=True, vmem_limit_bytes=60 * 2**20
            ),
        )(dilation, window, queries, key_heads, value_heads)

    return jax.shard_map(
        body,
        mesh=mesh,
        in_specs=(P("seq", "head"), P("seq", "head"), P("seq", "head"), P(), P()),
        out_specs=P("seq", "head"),
        check_vma=False,
    )
```
